32 devices in a mesh: groups: 2 (over y), assets: 8 (over z, x), tm: 2 (over core).
Axes of the slice: x: 2, y: 2, z: 4, core: 2. Of those that a mesh axis runs over, the one named last changes fastest.
Arguments:
- returns: bfloat16 [1536, 16384], P('tm', ('groups', 'assets')), parts along dimension 1, may hold values from -24 to 24
- prior: float32 [16384, 8192], P(('groups', 'assets')), parts along dimension 0, may hold values from -3 to 3
Outputs:
- covariance: float32 [2, 16384, 8192], P('tm', ('groups', 'assets')), parts along dimension 1
The draws below stay inside these ranges and needn't reach their ends.
There are 2 independent parts, one for each index of `groups`. The reference program is written for one: setup_inputs(seed, part) draws one part's arguments, and reference() takes and returns one part's arrays. A program takes and returns all parts, laid end to end along the dimension named above; each array names one. Nothing has to cross between parts.
All inputs are finite; a program needn't handle non-finite values.
Results may differ from the reference program's by a relative error of at most 0.0045.
Values may be sent and summed in bfloat16 or wider, within the bound.
A program may use at most 256 MiB of HBM per device.

```python
import jax
import jax.numpy as jnp
from jax import lax

ASSETS = 8192
MIN_DEV = 768
SLABS = 2
MINUTES = 1536


def block_levels(stream_key, dims, cuts, smallest, top_value):
    factor_of = 1.0
    for dim, blocks in cuts:
        steps = jax.random.uniform(jax.random.fold_in(jax.random.fold_in(stream_key, 6), dim), (blocks,), jnp.float32, smallest / len(cuts), top_value / len(cuts))
        factor_of = factor_of * jnp.repeat(jnp.exp(steps), dims[dim] // blocks).reshape((-1,) + (1,) * (len(dims) - 1 - dim))
    return factor_of


def scatter_about(stream_key, extent, width, reach, shards=(), held_as=jnp.bfloat16):
    drawn = jax.random.normal(stream_key, extent, jnp.float32) * width
    if len(shards) > 0:
        drawn = block_levels(stream_key, extent, shards, -0.22, 0.18) * drawn
    return jnp.clip(drawn, min=-reach, max=reach).astype(held_as)


def setup_inputs(seed: int = 0, part: int = 0) -> dict:
    streams_of = jax.random.split(jax.random.key(seed), 3)
    own_keys = jax.random.split(jax.random.fold_in(streams_of[2], part), 3)
    returns = scatter_about(own_keys[0], (MINUTES, ASSETS), 4.0, 24.0, ((0, 2), (1, 8)))
    prior = scatter_about(own_keys[1], (ASSETS, ASSETS), 0.5, 3.0, ((0, 8),), jnp.float32)
    return dict(returns=returns, prior=prior)


def reference(returns, prior):
    lam = jnp.float32(0.9995)
    position = jnp.arange(MIN_DEV, dtype=jnp.float32)
    weight = jnp.sqrt((jnp.float32(1.0) - lam) * jnp.power(lam, jnp.float32(MIN_DEV - 1) - position))
    factor = jnp.power(lam, jnp.float32(MIN_DEV))
    carry = prior
    results = []
    for slab in range(SLABS):
        piece = returns[slab * MIN_DEV:(slab + 1) * MIN_DEV]
        scaled = (piece.astype(jnp.float32) * weight[:, None]).astype(jnp.bfloat16).astype(jnp.float32)
        gram = jnp.dot(scaled.T, scaled, precision=lax.Precision.HIGHEST)
        carry = factor * carry + gram
        results.append(carry)
    return jnp.stack(results)
```

```python
import functools

import jax
import jax.numpy as jnp
from jax import lax
from jax.experimental import pallas as pl
from jax.experimental.pallas import tpu as pltpu
from jax.sharding import PartitionSpec as P

MESH = pl.DeviceIdType.MESH
PIECES = 4


def powers_of(minutes):
    lam = jnp.float32(0.9995)
    position = jnp.arange(minutes, dtype=jnp.float32)
    square = (jnp.float32(1.0) - lam) * jnp.power(lam, jnp.float32(minutes - 1) - position)
    return square, jnp.power(lam, jnp.float32(minutes))


def local_general(returns, prior):
    minutes, _ = returns.shape
    square, factor = powers_of(minutes)
    scaled = (returns.astype(jnp.float32) * jnp.sqrt(square)[:, None]).astype(jnp.bfloat16)
    tile = lax.dot_general(
        scaled,
        lax.all_gather(scaled, "assets", axis=1, tiled=True),
        (((0,), (0,)), ((), ())),
        preferred_element_type=jnp.float32,
    )
    mine = lax.axis_index("tm")
    everything = lax.all_gather(tile.astype(jnp.bfloat16), "tm")

    def turn(k, before):
        new = factor * before + everything[k].astype(jnp.float32)
        return jnp.where(k < mine, new, before)

    before = lax.fori_loop(0, lax.axis_size("tm"), turn, prior)
    return (factor * before + tile)[None]


def kernel(
    coef, returns, prior, square, total, mine, early, left, left_early,
    load_sem, prior_sem, x_send, z_send, c_send, f_send, x_recv, z_recv, c_recv, f_recv
):
    minutes, width = returns.shape
    part = width // PIECES
    me, core = lax.axis_index("assets"), lax.axis_index("tm")
    row, column = me // 2, me % 2
    other = 1 - column
    upper = row // 2
    outer = jnp.logical_or(row == 0, row == 3)
    inner = jnp.logical_not(outer)
    first, second = core == 0, core == 1
    line_row = lambda q: q + upper * (3 - 2 * q)
    block = lambda q, c: line_row(q) * 2 + c
    depth = (1 - upper) * row + upper * (3 - row)
    across = row * 2 + other
    beside = block(1 - depth, column)
    centre = (3 - row) * 2 + column

    barrier = pltpu.get_barrier_semaphore()
    for there in (across, beside):
        pl.semaphore_signal(barrier, 1, device_id={"assets": there}, device_id_type=MESH)
    pl.semaphore_signal(barrier, 1, device_id={"tm": 1 - core}, device_id_type=MESH)

    @pl.when(inner)
    def _():
        pl.semaphore_signal(barrier, 1, device_id={"assets": centre}, device_id_type=MESH)
        pl.semaphore_wait(barrier, 4)

    @pl.when(outer)
    def _():
        pl.semaphore_wait(barrier, 3)

    def remote(source, target, send, recv, where):
        return pltpu.make_async_remote_copy(
            src_ref=source, dst_ref=target, send_sem=send, recv_sem=recv,
            device_id=where, device_id_type=MESH,
        )

    def slot(j, p):
        return mine.at[j * PIECES + p]

    def send_x(source, j, p, k):
        remote(source, slot(j, p), x_send.at[k], x_recv.at[k], {"assets": across}).start()

    def send_z(source, j, p, k):
        remote(source, slot(j, p), z_send.at[k], z_recv.at[k], {"assets": beside}).start()

    def send_c(source, j, p, k):
        remote(source, slot(j, p), c_send.at[k], c_recv.at[k], {"assets": centre}).start()

    def hand_on(source, j, p):
        k = j * PIECES + p

        @pl.when(first)
        def _():
            remote(source, early.at[k], f_send.at[k], f_recv.at[k], {"tm": 1 - core}).start()

    def wait_recv(sem):
        pltpu.make_async_copy(mine.at[0], mine.at[0], sem).wait()

    def got(sem, j, p):
        wait_recv(sem)
        hand_on(slot(j, p), j, p)

    own = lambda p: returns.at[:, pl.ds(p * part, part)]

    for p in range(PIECES):
        send_x(own(p), me, p, p)
        send_z(own(p), me, p, p)

        @pl.when(inner)
        def _():
            send_c(own(p), me, p, p)

        hand_on(own(p), me, p)
        pltpu.make_async_copy(own(p), slot(me, p), load_sem.at[p]).start()

    blocks = total.shape[1] // width

    def prior_copy(j):
        columns = pl.ds(pl.multiple_of(j * width, width), width)
        return pltpu.make_async_copy(prior.at[:, columns], total.at[:, columns], prior_sem.at[j])

    def start_prior(j, carry):
        prior_copy(j).start()
        return carry

    lax.fori_loop(0, blocks, start_prior, 0)

    def prepare(p, carry):
        pltpu.make_async_copy(own(p), slot(me, p), load_sem.at[p]).wait()
        rows = pl.ds(pl.multiple_of(p * part, part), part)
        turned = mine[me * PIECES + p].astype(jnp.float32).T
        left[rows, :] = (turned * square[...]).astype(jnp.bfloat16)

        @pl.when(second)
        def _():
            k = me * PIECES + p
            wait_recv(f_recv.at[k])
            turned = early[k].astype(jnp.float32).T
            left_early[rows, :] = (turned * (coef[1] * square[...])).astype(jnp.bfloat16)

        return carry

    lax.fori_loop(0, PIECES, prepare, 0)

    def wait_prior(j, carry):
        prior_copy(j).wait()
        return carry

    lax.fori_loop(0, blocks, wait_prior, 0)

    def product(j, p, arrived=True):
        k = j * PIECES + p
        columns = pl.ds(pl.multiple_of(j * width + p * part, part), part)

        @pl.when(first)
        def _():
            total[:, columns] = coef[0] * total[:, columns] + jnp.dot(
                left[...], mine[k], preferred_element_type=jnp.float32
            )

        @pl.when(second)
        def _():
            if arrived:
                wait_recv(f_recv.at[k])
            total[:, columns] = (
                coef[0] * total[:, columns]
                + jnp.dot(left[...], mine[k], preferred_element_type=jnp.float32)
                + jnp.dot(left_early[...], early[k], preferred_element_type=jnp.float32)
            )

    def own_product(p, carry):
        product(me, p, arrived=False)
        return carry

    lax.fori_loop(0, PIECES, own_product, 0)

    @pl.when(outer)
    def _():
        def turn(k, carry):
            q, p = k // PIECES, k % PIECES
            jx, jz = block(q, other), block(1 + q, column)
            got(x_recv.at[k], jx, p)

            @pl.when(q == 0)
            def _():
                send_z(slot(jx, p), jx, p, PIECES + k)

            got(z_recv.at[k], jz, p)

            @pl.when(k < 10)
            def _():
                send_x(slot(jz, p), jz, p, PIECES + k)

            product(jx, p)
            product(jz, p)
            return carry

        lax.fori_loop(0, 3 * PIECES, turn, 0)

        def end(p, carry):
            j = block(3, other)
            got(x_recv.at[12 + p], j, p)
            got(z_recv.at[12 + p], j, 2 + p)
            product(j, p)
            product(j, 2 + p)
            return carry

        lax.fori_loop(0, 2, end, 0)

    @pl.when(inner)
    def _():
        def turn(k, carry):
            q, p = k // PIECES, k % PIECES
            jx, jz, jc = block(1 + q, other), block(0, (column + q) % 2), block(2 + q, column)
            got(c_recv.at[k], jc, p)
            send_z(slot(jc, p), jc, p, PIECES + k)
            send_x(slot(jc, p), jc, p, PIECES + k + q * (2 - 4 * (p // 2)))
            got(z_recv.at[k], jz, p)

            @pl.when(q == 0)
            def _():
                send_c(slot(jz, p), jz, p, PIECES + k)

            got(x_recv.at[k], jx, p)
            product(jc, p)
            product(jz, p)
            product(jx, p)
            return carry

        lax.fori_loop(0, 2 * PIECES, turn, 0)

        def end(k, carry):
            j, p = block(3, other), (k + 2) % PIECES
            got(x_recv.at[2 * PIECES + k], j, p)

            @pl.when(k < 2)
            def _():
                send_z(slot(j, p), j, p, 3 * PIECES + k)

            product(j, p)
            return carry

        lax.fori_loop(0, PIECES, end, 0)

    def wait_send(sem):
        pltpu.make_async_copy(mine.at[0], mine.at[0], sem).wait()

    def waits(sems, count):
        def turn(k, carry):
            wait_send(sems.at[k])
            return carry

        lax.fori_loop(0, count, turn, 0)

    @pl.when(outer)
    def _():
        waits(x_send, 14)
        waits(z_send, 8)

    @pl.when(inner)
    def _():
        waits(x_send, 12)
        waits(z_send, 14)
        waits(c_send, 8)

    @pl.when(first)
    def _():
        waits(f_send, blocks * PIECES)


def local_planned(returns, prior):
    minutes, width = returns.shape
    rows, assets = prior.shape
    part = width // PIECES
    square, factor = powers_of(minutes)
    slab = lax.axis_index("tm")
    coef = jnp.stack([jnp.where(slab > 0, factor * factor, factor), factor])
    count = assets // width * PIECES
    out = pl.pallas_call(
        kernel,
        out_shape=pltpu.VMEM((rows, assets), jnp.float32),
        in_specs=[
            pl.BlockSpec(memory_space=pltpu.SMEM),
            pl.BlockSpec(memory_space=pltpu.HBM),
            pl.BlockSpec(memory_space=pltpu.HBM),
            pl.BlockSpec(memory_space=pltpu.VMEM),
        ],
        out_specs=pl.BlockSpec(memory_space=pltpu.VMEM),
        scratch_shapes=[
            pltpu.VMEM((count, minutes, part), jnp.bfloat16),
            pltpu.VMEM((count, minutes, part), jnp.bfloat16),
            pltpu.VMEM((width, minutes), jnp.bfloat16),
            pltpu.VMEM((width, minutes), jnp.bfloat16),
            pltpu.SemaphoreType.DMA((PIECES,)),
            pltpu.SemaphoreType.DMA((assets // width,)),
            pltpu.SemaphoreType.DMA((14,)),
            pltpu.SemaphoreType.DMA((14,)),
            pltpu.SemaphoreType.DMA((8,)),
            pltpu.SemaphoreType.DMA((count,)),
            pltpu.SemaphoreType.DMA((14,)),
            pltpu.SemaphoreType.DMA((14,)),
            pltpu.SemaphoreType.DMA((8,)),
            pltpu.SemaphoreType.DMA((count,)),
        ],
        compiler_params=pltpu.CompilerParams(
            collective_id=0, has_side_effects=True, vmem_limit_bytes=31457280
        ),
    )(coef, pltpu.with_memory_space_constraint(returns, pltpu.HBM), prior, square[None, :])
    return out[None]


def solution(mesh):
    placed = (P("tm", ("groups", "assets")), P(("groups", "assets"), None))
    planned = mesh.shape["tm"] == 2 and mesh.shape["assets"] == 8

    def local(returns, prior):
        if planned and returns.shape[1] % (128 * PIECES) == 0 and returns.shape[0] % 128 == 0:
            return local_planned(returns, prior)
        return local_general(returns, prior)

    return jax.shard_map(
        local,
        mesh=mesh,
        in_specs=placed,
        out_specs=P("tm", ("groups", "assets"), None),
        check_vma=False,
    )
```

```python
import functools
import math

import jax
import jax.numpy as jnp
import numpy as np
from jax import lax
from jax.experimental import pallas as pl
from jax.experimental.pallas import tpu as pltpu
from jax.sharding import PartitionSpec as P

MESH = pl.DeviceIdType.MESH
PIECES = 4
HALF = PIECES // 2


def powers_of(minutes):
    lam = jnp.float32(0.9995)
    position = jnp.arange(minutes, dtype=jnp.float32)
    square = (jnp.float32(1.0) - lam) * jnp.power(lam, jnp.float32(minutes - 1) - position)
    return square, jnp.power(lam, jnp.float32(minutes))


def local_general(returns, prior):
    minutes, _ = returns.shape
    square, factor = powers_of(minutes)
    scaled = (returns.astype(jnp.float32) * jnp.sqrt(square)[:, None]).astype(jnp.bfloat16)
    tile = lax.dot_general(
        scaled,
        lax.all_gather(scaled, "assets", axis=1, tiled=True),
        (((0,), (0,)), ((), ())),
        preferred_element_type=jnp.float32,
    )
    mine = lax.axis_index("tm")
    everything = lax.all_gather(tile.astype(jnp.bfloat16), "tm")

    def turn(k, before):
        new = factor * before + everything[k].astype(jnp.float32)
        return jnp.where(k < mine, new, before)

    before = lax.fori_loop(0, lax.axis_size("tm"), turn, prior)
    return (factor * before + tile)[None]


def kernel(
    returns, prior, total, tail, left, hand, mine, early, left_early,
    load_sem, prior_sem, x_send, z_send, c_send, f_send, x_recv, z_recv, c_recv, f_recv
):
    minutes, width = returns.shape
    part = width // PIECES
    me, core = lax.axis_index("assets"), lax.axis_index("tm")
    row, column = me // 2, me % 2
    other = 1 - column
    upper = row // 2
    outer = jnp.logical_or(row == 0, row == 3)
    inner = jnp.logical_not(outer)
    first, second = core == 0, core == 1
    lam = float(np.float32(0.9995))
    factor = lam**minutes
    age = (minutes - 1) - lax.broadcasted_iota(jnp.int32, (1, minutes), 1)
    square = (1.0 - lam) * jnp.exp(age.astype(jnp.float32) * math.log(lam))
    line_row = lambda q: q + upper * (3 - 2 * q)
    block = lambda q, c: line_row(q) * 2 + c
    depth = (1 - upper) * row + upper * (3 - row)
    across = row * 2 + other
    beside = block(1 - depth, column)
    centre = (3 - row) * 2 + column

    barrier = pltpu.get_barrier_semaphore()
    for there in (across, beside):
        pl.semaphore_signal(barrier, 1, device_id={"assets": there}, device_id_type=MESH)
    pl.semaphore_signal(barrier, 1, device_id={"tm": 1 - core}, device_id_type=MESH)

    @pl.when(inner)
    def _():
        pl.semaphore_signal(barrier, 1, device_id={"assets": centre}, device_id_type=MESH)
        pl.semaphore_wait(barrier, 4)

    @pl.when(outer)
    def _():
        pl.semaphore_wait(barrier, 3)

    def remote(source, target, send, recv, where):
        return pltpu.make_async_remote_copy(
            src_ref=source, dst_ref=target, send_sem=send, recv_sem=recv,
            device_id=where, device_id_type=MESH,
        )

    def slot(j, p):
        return mine.at[j * PIECES + p]

    def send_x(source, j, p, k):
        remote(source, slot(j, p), x_send.at[k], x_recv.at[k], {"assets": across}).start()

    def send_z(source, j, p, k):
        remote(source, slot(j, p), z_send.at[k], z_recv.at[k], {"assets": beside}).start()

    def send_c(source, j, p, k):
        remote(source, slot(j, p), c_send.at[k], c_recv.at[k], {"assets": centre}).start()

    def hand_on(source, j, p):
        k = j * PIECES + p

        @pl.when(first)
        def _():
            remote(source, early.at[k], f_send.at[k], f_recv.at[k], {"tm": 1 - core}).start()

    def wait_recv(sem):
        pltpu.make_async_copy(mine.at[0], mine.at[0], sem).wait()

    def got(sem, j, p):
        wait_recv(sem)
        hand_on(slot(j, p), j, p)

    own = lambda p: returns.at[:, pl.ds(p * part, part)]

    for p in range(PIECES):
        send_x(own(p), me, p, p)
        send_z(own(p), me, p, p)

        @pl.when(inner)
        def _():
            send_c(own(p), me, p, p)

        hand_on(own(p), me, p)
        pltpu.make_async_copy(own(p), slot(me, p), load_sem.at[p]).start()

    blocks = prior.shape[1] // width
    last = block(3, other)
    place_of = lambda j: (j + blocks - 1 - last) % blocks

    def prior_copy(k):
        j = (last + 1 + k) % blocks
        columns = pl.ds(pl.multiple_of(j * width, width), width)
        return pltpu.make_async_copy(prior.at[:, columns], total.at[k], prior_sem.at[k])

    tail_copy = pltpu.make_async_copy(
        prior.at[:, pl.ds(pl.multiple_of(last * width, width), width)], tail, prior_sem.at[blocks - 1]
    )

    def start_prior(k, carry):
        prior_copy(k).start()
        return carry

    lax.fori_loop(0, blocks - 1, start_prior, 0)
    tail_copy.start()

    def prepare(p, carry):
        pltpu.make_async_copy(own(p), slot(me, p), load_sem.at[p]).wait()
        rows = pl.ds(pl.multiple_of(p * part, part), part)
        turned = mine[me * PIECES + p].astype(jnp.float32).T
        left[rows, :] = (turned * square).astype(jnp.bfloat16)

        @pl.when(second)
        def _():
            k = me * PIECES + p
            wait_recv(f_recv.at[k])
            turned = early[k].astype(jnp.float32).T
            left_early[rows, :] = (turned * (factor * square)).astype(jnp.bfloat16)

        return carry

    lax.fori_loop(0, PIECES, prepare, 0)

    def wait_prior(j, carry):
        prior_copy(j).wait()
        return carry

    lax.fori_loop(0, blocks - 1, wait_prior, 0)
    tail_copy.wait()

    def keep(j, p, k):
        return pltpu.make_async_copy(slot(j, p), hand.at[k], load_sem.at[k])

    def product(target, j, p, arrived=True, whole=True):
        k = j * PIECES + p
        columns = pl.ds(pl.multiple_of(p * part, part), part)

        @pl.when(first)
        def _():
            target[:, columns] = factor * target[:, columns] + jnp.dot(
                left[...], mine[k], preferred_element_type=jnp.float32
            )

        @pl.when(second)
        def _():
            if arrived:
                wait_recv(f_recv.at[k])
            now = factor * factor * target[:, columns] + jnp.dot(
                left_early[...], early[k], preferred_element_type=jnp.float32
            )
            if whole:
                now += jnp.dot(left[...], mine[k], preferred_element_type=jnp.float32)
            target[:, columns] = now

    def own_product(p, carry):
        product(total.at[place_of(me)], me, p, arrived=False)
        return carry

    lax.fori_loop(0, PIECES, own_product, 0)

    @pl.when(outer)
    def _():
        def turn(k, carry):
            q, p = k // PIECES, k % PIECES
            jx, jz = block(q, other), block(1 + q, column)
            got(x_recv.at[k], jx, p)

            @pl.when(q == 0)
            def _():
                send_z(slot(jx, p), jx, p, PIECES + k)

            got(z_recv.at[k], jz, p)
            late = jnp.logical_and(k >= 2 * PIECES, k < 2 * PIECES + HALF)

            @pl.when(jnp.logical_or(k < 2 * PIECES, jnp.logical_and(late, first)))
            def _():
                send_x(slot(jz, p), jz, p, PIECES + k)

            @pl.when(jnp.logical_and(late, second))
            def _():
                keep(jz, p, p).start()

            product(total.at[place_of(jx)], jx, p)
            product(total.at[place_of(jz)], jz, p)
            return carry

        lax.fori_loop(0, 3 * PIECES, turn, 0)

        def end(p, carry):
            j = block(3, other)

            @pl.when(first)
            def _():
                got(x_recv.at[3 * PIECES + p], j, p)
                got(z_recv.at[3 * PIECES + p], j, HALF + p)

            product(tail, j, p, whole=False)
            product(tail, j, HALF + p, whole=False)
            return carry

        lax.fori_loop(0, HALF, end, 0)

    @pl.when(inner)
    def _():
        def turn(k, carry):
            q, p = k // PIECES, k % PIECES
            jx, jz, jc = block(1 + q, other), block(0, (column + q) % 2), block(2 + q, column)
            got(c_recv.at[k], jc, p)
            send_z(slot(jc, p), jc, p, PIECES + k)
            send_x(slot(jc, p), jc, p, PIECES + k + q * HALF * (1 - 2 * (p // HALF)))
            got(z_recv.at[k], jz, p)

            @pl.when(q == 0)
            def _():
                send_c(slot(jz, p), jz, p, PIECES + k)

            got(x_recv.at[k], jx, p)
            product(total.at[place_of(jc)], jc, p)
            product(total.at[place_of(jz)], jz, p)
            product(total.at[place_of(jx)], jx, p)
            return carry

        lax.fori_loop(0, 2 * PIECES, turn, 0)

        def end(k, carry):
            j, p = block(3, other), (k + HALF) % PIECES
            got(x_recv.at[2 * PIECES + k], j, p)

            @pl.when(jnp.logical_and(k < HALF, first))
            def _():
                send_z(slot(j, p), j, p, 3 * PIECES + k)

            @pl.when(jnp.logical_and(k < HALF, second))
            def _():
                keep(j, p, k).start()

            product(tail, j, p)
            return carry

        lax.fori_loop(0, PIECES, end, 0)

    def wait_send(sem):
        pltpu.make_async_copy(mine.at[0], mine.at[0], sem).wait()

    def waits(sems, start, stop):
        def turn(k, carry):
            wait_send(sems.at[k])
            return carry

        lax.fori_loop(start, stop, turn, 0)

    waits(x_send, 0, 3 * PIECES)
    waits(z_send, 0, 2 * PIECES)

    @pl.when(inner)
    def _():
        waits(z_send, 2 * PIECES, 3 * PIECES)
        waits(c_send, 0, 2 * PIECES)

    @pl.when(first)
    def _():
        pl.when(outer)(lambda: waits(x_send, 3 * PIECES, 3 * PIECES + HALF))
        pl.when(inner)(lambda: waits(z_send, 3 * PIECES, 3 * PIECES + HALF))
        waits(f_send, 0, blocks * PIECES)

    @pl.when(second)
    def _():
        for k in range(HALF):
            keep(0, 0, k).wait()


def place():
    me = lax.axis_index("assets")
    row, column = me // 2, me % 2
    upper = row // 2
    outer = jnp.logical_or(row == 0, row == 3)
    last = 3 * (1 - upper) * 2 + 1 - column
    return outer, last


def write_kernel(total, out, sems):
    width = total.shape[2]
    blocks = out.shape[1] // width
    _, last = place()

    def piece(k):
        columns = pl.ds(pl.multiple_of((last + 1 + k) % blocks * width, width), width)
        return pltpu.make_async_copy(total.at[k], out.at[:, columns], sems.at[k])

    for k in range(blocks - 1):
        piece(k).start()
    for k in range(blocks - 1):
        piece(k).wait()


def write_most(total):
    blocks, rows, width = total.shape
    assets = (blocks + 1) * width
    return pl.pallas_call(
        write_kernel,
        out_shape=jax.ShapeDtypeStruct((rows, assets), total.dtype),
        in_specs=[pl.BlockSpec(memory_space=pltpu.VMEM)],
        out_specs=pl.BlockSpec(memory_space=pltpu.HBM),
        scratch_shapes=[pltpu.SemaphoreType.DMA((blocks,))],
        compiler_params=pltpu.CompilerParams(vmem_limit_bytes=1024 * 1024),
        cost_estimate=pl.CostEstimate(
            flops=0, bytes_accessed=8 * rows * assets, transcendentals=0
        ),
    )(total)


def finish_kernel(tail, left, from_x, from_z, held, out, stage, sems):
    width, part = left.shape[0], from_x.shape[2]
    outer, last = place()
    late = jnp.logical_and(outer, lax.axis_index("tm") == 1)
    start = pl.multiple_of(last * width, width)

    @pl.when(jnp.logical_not(late))
    def _():
        columns = pl.ds(start, width)
        copy = pltpu.make_async_copy(tail, out.at[:, columns], sems.at[0])
        copy.start()
        copy.wait()

    @pl.when(late)
    def _():
        copies = []
        for p in range(PIECES):
            source = from_x if p < HALF else from_z
            columns = pl.ds(pl.multiple_of(start + p * part, part), part)
            stage[p] = tail[:, pl.ds(p * part, part)] + jnp.dot(
                left[...], source[p % HALF], preferred_element_type=jnp.float32
            )
            copies.append(pltpu.make_async_copy(stage.at[p], out.at[:, columns], sems.at[p]))
            copies[-1].start()
        for copy in copies:
            copy.wait()


def finish(tail, left, from_x, from_z, held):
    rows = tail.shape[0]
    width, minutes = left.shape
    vmem, hbm = pl.BlockSpec(memory_space=pltpu.VMEM), pl.BlockSpec(memory_space=pltpu.HBM)
    return pl.pallas_call(
        finish_kernel,
        out_shape=jax.ShapeDtypeStruct(held.shape, held.dtype),
        in_specs=[vmem, vmem, vmem, vmem, hbm],
        out_specs=hbm,
        scratch_shapes=[
            pltpu.VMEM((PIECES, rows, width // PIECES), jnp.float32),
            pltpu.SemaphoreType.DMA((PIECES,)),
        ],
        input_output_aliases={4: 0},
        compiler_params=pltpu.CompilerParams(vmem_limit_bytes=10 * 1024 * 1024),
        cost_estimate=pl.CostEstimate(
            flops=2 * rows * width * minutes, bytes_accessed=4 * rows * width, transcendentals=0
        ),
    )(tail, left, from_x, from_z, held)


def local_planned(returns, prior):
    minutes, width = returns.shape
    rows, assets = prior.shape
    part = width // PIECES
    count = assets // width * PIECES
    hbm, vmem = pl.BlockSpec(memory_space=pltpu.HBM), pl.BlockSpec(memory_space=pltpu.VMEM)
    semaphores = [PIECES, assets // width]
    semaphores += 2 * [3 * PIECES + HALF, 3 * PIECES + HALF, 2 * PIECES, count]
    total, tail, left, hand = pl.pallas_call(
        kernel,
        out_shape=(
            pltpu.VMEM((assets // width - 1, rows, width), jnp.float32),
            pltpu.VMEM((rows, width), jnp.float32),
            pltpu.VMEM((width, minutes), jnp.bfloat16),
            pltpu.HBM((HALF, minutes, part), jnp.bfloat16),
        ),
        in_specs=[hbm, hbm],
        out_specs=(vmem, vmem, vmem, hbm),
        scratch_shapes=[
            pltpu.VMEM((count, minutes, part), jnp.bfloat16),
            pltpu.VMEM((count, minutes, part), jnp.bfloat16),
            pltpu.VMEM((width, minutes), jnp.bfloat16),
            *[pltpu.SemaphoreType.DMA((n,)) for n in semaphores],
        ],
        compiler_params=pltpu.CompilerParams(
            collective_id=0, has_side_effects=True, vmem_limit_bytes=29 * 1024 * 1024
        ),
    )(pltpu.with_memory_space_constraint(returns, pltpu.HBM), prior)
    at = lambda row, column: (row * 2 + column) * 2 + 1
    pairs_x = [(at(r, c), at(r, 1 - c)) for r in (0, 3) for c in (0, 1)]
    pairs_z = [(at(n, c), at(r, c)) for r, n in ((0, 1), (3, 2)) for c in (0, 1)]
    from_x = lax.ppermute(hand, ("assets", "tm"), pairs_x)
    from_z = lax.ppermute(hand, ("assets", "tm"), pairs_z)
    return finish(tail, left, from_x, from_z, write_most(total))[None]


def solution(mesh):
    placed = (P("tm", ("groups", "assets")), P(("groups", "assets"), None))
    planned = mesh.shape["tm"] == 2 and mesh.shape["assets"] == 8

    def local(returns, prior):
        if planned and returns.shape[1] % (128 * PIECES) == 0 and returns.shape[0] % 128 == 0:
            return local_planned(returns, prior)
        return local_general(returns, prior)

    return jax.shard_map(
        local,
        mesh=mesh,
        in_specs=placed,
        out_specs=P("tm", ("groups", "assets"), None),
        check_vma=False,
    )
```

```python
import functools
import math

import jax
import jax.numpy as jnp
import numpy as np
from jax import lax
from jax.experimental import pallas as pl
from jax.experimental.pallas import tpu as pltpu
from jax.sharding import PartitionSpec as P

MESH = pl.DeviceIdType.MESH
PIECES = 4
HALF = PIECES // 2


def powers_of(minutes):
    lam = jnp.float32(0.9995)
    position = jnp.arange(minutes, dtype=jnp.float32)
    square = (jnp.float32(1.0) - lam) * jnp.power(lam, jnp.float32(minutes - 1) - position)
    return square, jnp.power(lam, jnp.float32(minutes))


def local_general(returns, prior):
    minutes, _ = returns.shape
    square, factor = powers_of(minutes)
    scaled = (returns.astype(jnp.float32) * jnp.sqrt(square)[:, None]).astype(jnp.bfloat16)
    tile = lax.dot_general(
        scaled,
        lax.all_gather(scaled, "assets", axis=1, tiled=True),
        (((0,), (0,)), ((), ())),
        preferred_element_type=jnp.float32,
    )
    mine = lax.axis_index("tm")
    everything = lax.all_gather(tile.astype(jnp.bfloat16), "tm")

    def turn(k, before):
        new = factor * before + everything[k].astype(jnp.float32)
        return jnp.where(k < mine, new, before)

    before = lax.fori_loop(0, lax.axis_size("tm"), turn, prior)
    return (factor * before + tile)[None]


def kernel(
    returns, prior, total, tail, left, hand, mine, early, left_early,
    load_sem, prior_sem, send_sem, x_recv, z_recv, c_recv, f_recv
):
    minutes, width = returns.shape
    part = width // PIECES
    me, core = lax.axis_index("assets"), lax.axis_index("tm")
    row, column = me // 2, me % 2
    other = 1 - column
    upper = row // 2
    outer = jnp.logical_or(row == 0, row == 3)
    inner = jnp.logical_not(outer)
    first, second = core == 0, core == 1
    lam = float(np.float32(0.9995))
    factor = lam**minutes
    age = (minutes - 1) - lax.broadcasted_iota(jnp.int32, (1, minutes), 1)
    square = (1.0 - lam) * jnp.exp(age.astype(jnp.float32) * math.log(lam))
    line_row = lambda q: q + upper * (3 - 2 * q)
    block = lambda q, c: line_row(q) * 2 + c
    depth = (1 - upper) * row + upper * (3 - row)
    across = row * 2 + other
    beside = block(1 - depth, column)
    centre = (3 - row) * 2 + column

    barrier = pltpu.get_barrier_semaphore()
    for there in (across, beside):
        pl.semaphore_signal(barrier, 1, device_id={"assets": there}, device_id_type=MESH)
    pl.semaphore_signal(barrier, 1, device_id={"tm": 1 - core}, device_id_type=MESH)

    @pl.when(inner)
    def _():
        pl.semaphore_signal(barrier, 1, device_id={"assets": centre}, device_id_type=MESH)
        pl.semaphore_wait(barrier, 4)

    @pl.when(outer)
    def _():
        pl.semaphore_wait(barrier, 3)

    def remote(source, target, send, recv, where):
        return pltpu.make_async_remote_copy(
            src_ref=source, dst_ref=target, send_sem=send, recv_sem=recv,
            device_id=where, device_id_type=MESH,
        )

    def slot(j, p):
        return mine.at[j * PIECES + p]

    def send_x(source, j, p, k):
        remote(source, slot(j, p), send_sem.at[0], x_recv.at[k], {"assets": across}).start()

    def send_z(source, j, p, k):
        remote(source, slot(j, p), send_sem.at[1], z_recv.at[k], {"assets": beside}).start()

    def send_c(source, j, p, k):
        remote(source, slot(j, p), send_sem.at[2], c_recv.at[k], {"assets": centre}).start()

    def hand_on(source, j, p):
        k = j * PIECES + p

        @pl.when(first)
        def _():
            remote(source, early.at[k], send_sem.at[3], f_recv.at[k], {"tm": 1 - core}).start()

    def wait_recv(sem):
        pltpu.make_async_copy(mine.at[0], mine.at[0], sem).wait()

    def wait_all(sem, count):
        pieces = mine.at[pl.ds(0, count)]
        pltpu.make_async_copy(pieces, pieces, sem).wait()

    def got(sem, j, p):
        wait_recv(sem)
        hand_on(slot(j, p), j, p)

    own = lambda p: returns.at[:, pl.ds(p * part, part)]

    for p in range(PIECES):
        send_x(own(p), me, p, p)
        send_z(own(p), me, p, p)

        @pl.when(inner)
        def _():
            send_c(own(p), me, p, p)

        hand_on(own(p), me, p)
        pltpu.make_async_copy(own(p), slot(me, p), load_sem.at[0]).start()

    blocks = prior.shape[1] // width
    last = block(3, other)
    place_of = lambda j: (j + blocks - 1 - last) % blocks

    def prior_copy(k):
        j = (last + 1 + k) % blocks
        columns = pl.ds(pl.multiple_of(j * width, width), width)
        return pltpu.make_async_copy(prior.at[:, columns], total.at[k], prior_sem.at[0])

    tail_copy = pltpu.make_async_copy(
        prior.at[:, pl.ds(pl.multiple_of(last * width, width), width)], tail, prior_sem.at[1]
    )

    def start_prior(k, carry):
        prior_copy(k).start()
        return carry

    lax.fori_loop(0, blocks - 1, start_prior, 0)
    tail_copy.start()

    def prepare(p, carry):
        rows = pl.ds(pl.multiple_of(p * part, part), part)
        turned = mine[me * PIECES + p].astype(jnp.float32).T
        left[rows, :] = (turned * square).astype(jnp.bfloat16)

        @pl.when(second)
        def _():
            k = me * PIECES + p
            wait_recv(f_recv.at[k])
            turned = early[k].astype(jnp.float32).T
            left_early[rows, :] = (turned * (factor * square)).astype(jnp.bfloat16)

        return carry

    wait_all(load_sem.at[0], PIECES)
    lax.fori_loop(0, PIECES, prepare, 0)

    pltpu.make_async_copy(total, total, prior_sem.at[0]).wait()
    tail_copy.wait()

    def keep(j, p, k):
        return pltpu.make_async_copy(slot(j, p), hand.at[k], load_sem.at[0])

    def product(target, j, p, arrived=True, whole=True):
        k = j * PIECES + p
        columns = pl.ds(pl.multiple_of(p * part, part), part)

        @pl.when(first)
        def _():
            target[:, columns] = factor * target[:, columns] + jnp.dot(
                left[...], mine[k], preferred_element_type=jnp.float32
            )

        @pl.when(second)
        def _():
            if arrived:
                wait_recv(f_recv.at[k])
            now = factor * factor * target[:, columns] + jnp.dot(
                left_early[...], early[k], preferred_element_type=jnp.float32
            )
            if whole:
                now += jnp.dot(left[...], mine[k], preferred_element_type=jnp.float32)
            target[:, columns] = now

    def own_product(p, carry):
        product(total.at[place_of(me)], me, p, arrived=False)
        return carry

    lax.fori_loop(0, PIECES, own_product, 0)

    @pl.when(outer)
    def _():
        def turn(k, carry):
            q, p = k // PIECES, k % PIECES
            jx, jz = block(q, other), block(1 + q, column)
            got(x_recv.at[k], jx, p)

            @pl.when(q == 0)
            def _():
                send_z(slot(jx, p), jx, p, PIECES + k)

            got(z_recv.at[k], jz, p)
            late = jnp.logical_and(k >= 2 * PIECES, k < 2 * PIECES + HALF)

            @pl.when(jnp.logical_or(k < 2 * PIECES, jnp.logical_and(late, first)))
            def _():
                send_x(slot(jz, p), jz, p, PIECES + k)

            @pl.when(jnp.logical_and(late, second))
            def _():
                keep(jz, p, p).start()

            product(total.at[place_of(jx)], jx, p)
            product(total.at[place_of(jz)], jz, p)
            return carry

        lax.fori_loop(0, 3 * PIECES, turn, 0)

        def end(p, carry):
            j = block(3, other)

            @pl.when(first)
            def _():
                got(x_recv.at[3 * PIECES + p], j, p)
                got(z_recv.at[3 * PIECES + p], j, HALF + p)

            product(tail, j, p, whole=False)
            product(tail, j, HALF + p, whole=False)
            return carry

        lax.fori_loop(0, HALF, end, 0)

    @pl.when(inner)
    def _():
        def turn(k, carry):
            q, p = k // PIECES, k % PIECES
            jx, jz, jc = block(1 + q, other), block(0, (column + q) % 2), block(2 + q, column)
            got(c_recv.at[k], jc, p)
            send_z(slot(jc, p), jc, p, PIECES + k)
            send_x(slot(jc, p), jc, p, PIECES + k + q * HALF * (1 - 2 * (p // HALF)))
            got(z_recv.at[k], jz, p)

            @pl.when(q == 0)
            def _():
                send_c(slot(jz, p), jz, p, PIECES + k)

            got(x_recv.at[k], jx, p)
            product(total.at[place_of(jc)], jc, p)
            product(total.at[place_of(jz)], jz, p)
            product(total.at[place_of(jx)], jx, p)
            return carry

        lax.fori_loop(0, 2 * PIECES, turn, 0)

        def end(k, carry):
            j, p = block(3, other), (k + HALF) % PIECES
            got(x_recv.at[2 * PIECES + k], j, p)

            @pl.when(jnp.logical_and(k < HALF, first))
            def _():
                send_z(slot(j, p), j, p, 3 * PIECES + k)

            @pl.when(jnp.logical_and(k < HALF, second))
            def _():
                keep(j, p, k).start()

            product(tail, j, p)
            return carry

        lax.fori_loop(0, PIECES, end, 0)

    @pl.when(outer)
    def _():
        wait_all(send_sem.at[1], 2 * PIECES)
        pl.when(first)(lambda: wait_all(send_sem.at[0], 3 * PIECES + HALF))
        pl.when(second)(lambda: wait_all(send_sem.at[0], 3 * PIECES))

    @pl.when(inner)
    def _():
        wait_all(send_sem.at[0], 3 * PIECES)
        wait_all(send_sem.at[2], 2 * PIECES)
        pl.when(first)(lambda: wait_all(send_sem.at[1], 3 * PIECES + HALF))
        pl.when(second)(lambda: wait_all(send_sem.at[1], 3 * PIECES))

    pl.when(first)(lambda: wait_all(send_sem.at[3], blocks * PIECES))
    pl.when(second)(lambda: wait_all(load_sem.at[0], HALF))


def place():
    me = lax.axis_index("assets")
    row, column = me // 2, me % 2
    upper = row // 2
    outer = jnp.logical_or(row == 0, row == 3)
    last = 3 * (1 - upper) * 2 + 1 - column
    return outer, last


def write_kernel(total, out, sems):
    width = total.shape[2]
    blocks = out.shape[1] // width
    _, last = place()

    def piece(k):
        columns = pl.ds(pl.multiple_of((last + 1 + k) % blocks * width, width), width)
        return pltpu.make_async_copy(total.at[k], out.at[:, columns], sems.at[k])

    for k in range(blocks - 1):
        piece(k).start()
    for k in range(blocks - 1):
        piece(k).wait()


def write_most(total):
    blocks, rows, width = total.shape
    assets = (blocks + 1) * width
    return pl.pallas_call(
        write_kernel,
        out_shape=jax.ShapeDtypeStruct((rows, assets), total.dtype),
        in_specs=[pl.BlockSpec(memory_space=pltpu.VMEM)],
        out_specs=pl.BlockSpec(memory_space=pltpu.HBM),
        scratch_shapes=[pltpu.SemaphoreType.DMA((blocks,))],
        compiler_params=pltpu.CompilerParams(vmem_limit_bytes=1024 * 1024),
        cost_estimate=pl.CostEstimate(
            flops=0, bytes_accessed=8 * rows * assets, transcendentals=0
        ),
    )(total)


def finish_kernel(tail, left, from_x, from_z, held, out, stage, sems):
    width, part = left.shape[0], from_x.shape[2]
    outer, last = place()
    late = jnp.logical_and(outer, lax.axis_index("tm") == 1)
    start = pl.multiple_of(last * width, width)

    @pl.when(jnp.logical_not(late))
    def _():
        columns = pl.ds(start, width)
        copy = pltpu.make_async_copy(tail, out.at[:, columns], sems.at[0])
        copy.start()
        copy.wait()

    @pl.when(late)
    def _():
        copies = []
        for p in range(PIECES):
            source = from_x if p < HALF else from_z
            columns = pl.ds(pl.multiple_of(start + p * part, part), part)
            stage[p] = tail[:, pl.ds(p * part, part)] + jnp.dot(
                left[...], source[p % HALF], preferred_element_type=jnp.float32
            )
            copies.append(pltpu.make_async_copy(stage.at[p], out.at[:, columns], sems.at[p]))
            copies[-1].start()
        for copy in copies:
            copy.wait()


def finish(tail, left, from_x, from_z, held):
    rows = tail.shape[0]
    width, minutes = left.shape
    vmem, hbm = pl.BlockSpec(memory_space=pltpu.VMEM), pl.BlockSpec(memory_space=pltpu.HBM)
    return pl.pallas_call(
        finish_kernel,
        out_shape=jax.ShapeDtypeStruct(held.shape, held.dtype),
        in_specs=[vmem, vmem, vmem, vmem, hbm],
        out_specs=hbm,
        scratch_shapes=[
            pltpu.VMEM((PIECES, rows, width // PIECES), jnp.float32),
            pltpu.SemaphoreType.DMA((PIECES,)),
        ],
        input_output_aliases={4: 0},
        compiler_params=pltpu.CompilerParams(vmem_limit_bytes=10 * 1024 * 1024),
        cost_estimate=pl.CostEstimate(
            flops=2 * rows * width * minutes, bytes_accessed=4 * rows * width, transcendentals=0
        ),
    )(tail, left, from_x, from_z, held)


def local_planned(returns, prior):
    minutes, width = returns.shape
    rows, assets = prior.shape
    part = width // PIECES
    count = assets // width * PIECES
    hbm, vmem = pl.BlockSpec(memory_space=pltpu.HBM), pl.BlockSpec(memory_space=pltpu.VMEM)
    semaphores = [1, 2, 4, 3 * PIECES + HALF, 3 * PIECES + HALF, 2 * PIECES, count]
    total, tail, left, hand = pl.pallas_call(
        kernel,
        out_shape=(
            pltpu.VMEM((assets // width - 1, rows, width), jnp.float32),
            pltpu.VMEM((rows, width), jnp.float32),
            pltpu.VMEM((width, minutes), jnp.bfloat16),
            pltpu.HBM((HALF, minutes, part), jnp.bfloat16),
        ),
        in_specs=[hbm, hbm],
        out_specs=(vmem, vmem, vmem, hbm),
        scratch_shapes=[
            pltpu.VMEM((count, minutes, part), jnp.bfloat16),
            pltpu.VMEM((count, minutes, part), jnp.bfloat16),
            pltpu.VMEM((width, minutes), jnp.bfloat16),
            *[pltpu.SemaphoreType.DMA((n,)) for n in semaphores],
        ],
        compiler_params=pltpu.CompilerParams(
            collective_id=0, has_side_effects=True, vmem_limit_bytes=29 * 1024 * 1024
        ),
    )(pltpu.with_memory_space_constraint(returns, pltpu.HBM), prior)
    at = lambda row, column: (row * 2 + column) * 2 + 1
    pairs_x = [(at(r, c), at(r, 1 - c)) for r in (0, 3) for c in (0, 1)]
    pairs_z = [(at(n, c), at(r, c)) for r, n in ((0, 1), (3, 2)) for c in (0, 1)]
    from_x = lax.ppermute(hand, ("assets", "tm"), pairs_x)
    from_z = lax.ppermute(hand, ("assets", "tm"), pairs_z)
    return finish(tail, left, from_x, from_z, write_most(total))[None]


def solution(mesh):
    placed = (P("tm", ("groups", "assets")), P(("groups", "assets"), None))
    planned = mesh.shape["tm"] == 2 and mesh.shape["assets"] == 8

    def local(returns, prior):
        if planned and returns.shape[1] % (128 * PIECES) == 0 and returns.shape[0] % 128 == 0:
            return local_planned(returns, prior)
        return local_general(returns, prior)

    return jax.shard_map(
        local,
        mesh=mesh,
        in_specs=placed,
        out_specs=P("tm", ("groups", "assets"), None),
        check_vma=False,
    )
```

```python
import functools
import math

import jax
import jax.numpy as jnp
import numpy as np
from jax import lax
from jax.experimental import pallas as pl
from jax.experimental.pallas import tpu as pltpu
from jax.sharding import PartitionSpec as P

MESH = pl.DeviceIdType.MESH
PIECES = 4
HALF = PIECES // 2


def powers_of(minutes):
    lam = jnp.float32(0.9995)
    position = jnp.arange(minutes, dtype=jnp.float32)
    square = (jnp.float32(1.0) - lam) * jnp.power(lam, jnp.float32(minutes - 1) - position)
    return square, jnp.power(lam, jnp.float32(minutes))


def local_general(returns, prior):
    minutes, _ = returns.shape
    square, factor = powers_of(minutes)
    scaled = (returns.astype(jnp.float32) * jnp.sqrt(square)[:, None]).astype(jnp.bfloat16)
    tile = lax.dot_general(
        scaled,
        lax.all_gather(scaled, "assets", axis=1, tiled=True),
        (((0,), (0,)), ((), ())),
        preferred_element_type=jnp.float32,
    )
    mine = lax.axis_index("tm")
    everything = lax.all_gather(tile.astype(jnp.bfloat16), "tm")

    def turn(k, before):
        new = factor * before + everything[k].astype(jnp.float32)
        return jnp.where(k < mine, new, before)

    before = lax.fori_loop(0, lax.axis_size("tm"), turn, prior)
    return (factor * before + tile)[None]


def kernel(
    returns, prior, total, tail, left, left_early, hand, rest, mine, early,
    load_sem, prior_sem, send_sem, x_recv, z_recv, c_recv, f_recv
):
    minutes, width = returns.shape
    part = width // PIECES
    me, core = lax.axis_index("assets"), lax.axis_index("tm")
    row, column = me // 2, me % 2
    other = 1 - column
    upper = row // 2
    outer = jnp.logical_or(row == 0, row == 3)
    inner = jnp.logical_not(outer)
    first, second = core == 0, core == 1
    lam = float(np.float32(0.9995))
    factor = lam**minutes
    age = (minutes - 1) - lax.broadcasted_iota(jnp.int32, (1, minutes), 1)
    square = (1.0 - lam) * jnp.exp(age.astype(jnp.float32) * math.log(lam))
    line_row = lambda q: q + upper * (3 - 2 * q)
    block = lambda q, c: line_row(q) * 2 + c
    depth = (1 - upper) * row + upper * (3 - row)
    across = row * 2 + other
    beside = block(1 - depth, column)
    centre = (3 - row) * 2 + column

    barrier = pltpu.get_barrier_semaphore()
    for there in (across, beside):
        pl.semaphore_signal(barrier, 1, device_id={"assets": there}, device_id_type=MESH)
    pl.semaphore_signal(barrier, 1, device_id={"tm": 1 - core}, device_id_type=MESH)

    @pl.when(inner)
    def _():
        pl.semaphore_signal(barrier, 1, device_id={"assets": centre}, device_id_type=MESH)
        pl.semaphore_wait(barrier, 4)

    @pl.when(outer)
    def _():
        pl.semaphore_wait(barrier, 3)

    def remote(source, target, send, recv, where):
        return pltpu.make_async_remote_copy(
            src_ref=source, dst_ref=target, send_sem=send, recv_sem=recv,
            device_id=where, device_id_type=MESH,
        )

    def slot(j, p):
        return mine.at[j * PIECES + p]

    def send_x(source, j, p, k):
        remote(source, slot(j, p), send_sem.at[0], x_recv.at[k], {"assets": across}).start()

    def send_z(source, j, p, k):
        remote(source, slot(j, p), send_sem.at[1], z_recv.at[k], {"assets": beside}).start()

    def send_c(source, j, p, k):
        remote(source, slot(j, p), send_sem.at[2], c_recv.at[k], {"assets": centre}).start()

    def hand_on(source, j, p):
        k = j * PIECES + p

        @pl.when(first)
        def _():
            remote(source, early.at[k], send_sem.at[3], f_recv.at[k], {"tm": 1 - core}).start()

    def wait_recv(sem):
        pltpu.make_async_copy(mine.at[0], mine.at[0], sem).wait()

    def wait_all(sem, count):
        pieces = mine.at[pl.ds(0, count)]
        pltpu.make_async_copy(pieces, pieces, sem).wait()

    def got(sem, j, p):
        wait_recv(sem)
        hand_on(slot(j, p), j, p)

    own = lambda p: returns.at[:, pl.ds(p * part, part)]

    for p in range(PIECES):
        send_x(own(p), me, p, p)
        send_z(own(p), me, p, p)

        @pl.when(inner)
        def _():
            send_c(own(p), me, p, p)

        hand_on(own(p), me, p)
        pltpu.make_async_copy(own(p), slot(me, p), load_sem.at[0]).start()

    blocks = prior.shape[1] // width
    last = block(3, other)
    place_of = lambda j: (j + blocks - 1 - last) % blocks

    def prior_copy(k):
        j = (last + 1 + k) % blocks
        columns = pl.ds(pl.multiple_of(j * width, width), width)
        return pltpu.make_async_copy(prior.at[:, columns], total.at[k], prior_sem.at[0])

    tail_copy = pltpu.make_async_copy(
        prior.at[:, pl.ds(pl.multiple_of(last * width, width), width)], tail, prior_sem.at[1]
    )

    def start_prior(k, carry):
        prior_copy(k).start()
        return carry

    lax.fori_loop(0, blocks - 1, start_prior, 0)
    tail_copy.start()

    def prepare(p, carry):
        rows = pl.ds(pl.multiple_of(p * part, part), part)
        turned = mine[me * PIECES + p].astype(jnp.float32).T
        left[rows, :] = (turned * square).astype(jnp.bfloat16)

        @pl.when(second)
        def _():
            k = me * PIECES + p
            wait_recv(f_recv.at[k])
            turned = early[k].astype(jnp.float32).T
            left_early[rows, :] = (turned * (factor * square)).astype(jnp.bfloat16)

        return carry

    wait_all(load_sem.at[0], PIECES)
    lax.fori_loop(0, PIECES, prepare, 0)

    pltpu.make_async_copy(total, total, prior_sem.at[0]).wait()
    tail_copy.wait()

    def keep(j, p, k):
        return pltpu.make_async_copy(slot(j, p), hand.at[k], load_sem.at[0])

    def product(target, j, p, arrived=True):
        k = j * PIECES + p
        columns = pl.ds(pl.multiple_of(p * part, part), part)

        @pl.when(first)
        def _():
            target[:, columns] = factor * target[:, columns] + jnp.dot(
                left[...], mine[k], preferred_element_type=jnp.float32
            )

        @pl.when(second)
        def _():
            if arrived:
                wait_recv(f_recv.at[k])
            now = factor * factor * target[:, columns] + jnp.dot(
                left_early[...], early[k], preferred_element_type=jnp.float32
            )
            now += jnp.dot(left[...], mine[k], preferred_element_type=jnp.float32)
            target[:, columns] = now

    def own_product(p, carry):
        product(total.at[place_of(me)], me, p, arrived=False)
        return carry

    lax.fori_loop(0, PIECES, own_product, 0)

    @pl.when(outer)
    def _():
        def turn(k, carry):
            q, p = k // PIECES, k % PIECES
            jx, jz = block(q, other), block(1 + q, column)
            got(x_recv.at[k], jx, p)

            @pl.when(q == 0)
            def _():
                send_z(slot(jx, p), jx, p, PIECES + k)

            got(z_recv.at[k], jz, p)
            late = jnp.logical_and(k >= 2 * PIECES, k < 2 * PIECES + HALF)

            @pl.when(jnp.logical_or(k < 2 * PIECES, jnp.logical_and(late, first)))
            def _():
                send_x(slot(jz, p), jz, p, PIECES + k)

            @pl.when(jnp.logical_and(late, second))
            def _():
                keep(jz, p, p).start()

            product(total.at[place_of(jx)], jx, p)
            product(total.at[place_of(jz)], jz, p)
            return carry

        lax.fori_loop(0, 3 * PIECES, turn, 0)

        @pl.when(first)
        def _():
            j = block(3, other)

            def end(i, carry):
                for sem, p in ((x_recv, i), (z_recv, HALF + i)):
                    wait_recv(sem.at[3 * PIECES + i])
                    pltpu.make_async_copy(slot(j, p), rest.at[p], load_sem.at[p]).start()
                for p in (i, HALF + i):
                    columns = pl.ds(pl.multiple_of(p * part, part), part)
                    tail[:, columns] = factor * tail[:, columns] + jnp.dot(
                        left[...], mine[j * PIECES + p], preferred_element_type=jnp.float32
                    )
                return carry

            lax.fori_loop(0, HALF, end, 0)
            for p in range(PIECES):
                wait_recv(load_sem.at[p])

        @pl.when(second)
        def _():
            def fade(p, carry):
                columns = pl.ds(pl.multiple_of(p * part, part), part)
                tail[:, columns] = factor * factor * tail[:, columns]
                return carry

            lax.fori_loop(0, PIECES, fade, 0)

    @pl.when(inner)
    def _():
        def turn(k, carry):
            q, p = k // PIECES, k % PIECES
            jx, jz, jc = block(1 + q, other), block(0, (column + q) % 2), block(2 + q, column)
            got(c_recv.at[k], jc, p)
            send_z(slot(jc, p), jc, p, PIECES + k)
            send_x(slot(jc, p), jc, p, PIECES + k + q * HALF * (1 - 2 * (p // HALF)))
            got(z_recv.at[k], jz, p)

            @pl.when(q == 0)
            def _():
                send_c(slot(jz, p), jz, p, PIECES + k)

            got(x_recv.at[k], jx, p)
            product(total.at[place_of(jc)], jc, p)
            product(total.at[place_of(jz)], jz, p)
            product(total.at[place_of(jx)], jx, p)
            return carry

        lax.fori_loop(0, 2 * PIECES, turn, 0)

        def end(k, carry):
            j, p = block(3, other), (k + HALF) % PIECES
            got(x_recv.at[2 * PIECES + k], j, p)

            @pl.when(jnp.logical_and(k < HALF, first))
            def _():
                send_z(slot(j, p), j, p, 3 * PIECES + k)

            @pl.when(jnp.logical_and(k < HALF, second))
            def _():
                keep(j, p, k).start()

            product(tail, j, p)
            return carry

        lax.fori_loop(0, PIECES, end, 0)

    @pl.when(outer)
    def _():
        wait_all(send_sem.at[1], 2 * PIECES)
        pl.when(first)(lambda: wait_all(send_sem.at[0], 3 * PIECES + HALF))
        pl.when(second)(lambda: wait_all(send_sem.at[0], 3 * PIECES))

    @pl.when(inner)
    def _():
        wait_all(send_sem.at[0], 3 * PIECES)
        wait_all(send_sem.at[2], 2 * PIECES)
        pl.when(first)(lambda: wait_all(send_sem.at[1], 3 * PIECES + HALF))
        pl.when(second)(lambda: wait_all(send_sem.at[1], 3 * PIECES))

    pl.when(jnp.logical_and(first, outer))(lambda: wait_all(send_sem.at[3], (blocks - 1) * PIECES))
    pl.when(jnp.logical_and(first, inner))(lambda: wait_all(send_sem.at[3], blocks * PIECES))
    pl.when(second)(lambda: wait_all(load_sem.at[0], HALF))


def place():
    me = lax.axis_index("assets")
    row, column = me // 2, me % 2
    upper = row // 2
    outer = jnp.logical_or(row == 0, row == 3)
    last = 3 * (1 - upper) * 2 + 1 - column
    return outer, last


def write_kernel(total, out, sems):
    width = total.shape[2]
    blocks = out.shape[1] // width
    _, last = place()

    def piece(k):
        columns = pl.ds(pl.multiple_of((last + 1 + k) % blocks * width, width), width)
        return pltpu.make_async_copy(total.at[k], out.at[:, columns], sems.at[k])

    for k in range(blocks - 1):
        piece(k).start()
    for k in range(blocks - 1):
        piece(k).wait()


def write_most(total):
    blocks, rows, width = total.shape
    assets = (blocks + 1) * width
    return pl.pallas_call(
        write_kernel,
        out_shape=jax.ShapeDtypeStruct((rows, assets), total.dtype),
        in_specs=[pl.BlockSpec(memory_space=pltpu.VMEM)],
        out_specs=pl.BlockSpec(memory_space=pltpu.HBM),
        scratch_shapes=[pltpu.SemaphoreType.DMA((blocks,))],
        compiler_params=pltpu.CompilerParams(vmem_limit_bytes=1024 * 1024),
        cost_estimate=pl.CostEstimate(
            flops=0, bytes_accessed=8 * rows * assets, transcendentals=0
        ),
    )(total)


def finish_kernel(tail, left, left_early, from_x, from_z, from_core, held, out, stage, sems):
    width, part = left.shape[0], from_x.shape[2]
    outer, last = place()
    late = jnp.logical_and(outer, lax.axis_index("tm") == 1)
    start = pl.multiple_of(last * width, width)

    @pl.when(jnp.logical_not(late))
    def _():
        columns = pl.ds(start, width)
        copy = pltpu.make_async_copy(tail, out.at[:, columns], sems.at[0])
        copy.start()
        copy.wait()

    @pl.when(late)
    def _():
        copies = []
        for p in range(PIECES):
            source = from_x if p < HALF else from_z
            columns = pl.ds(pl.multiple_of(start + p * part, part), part)
            stage[p] = (
                tail[:, pl.ds(p * part, part)]
                + jnp.dot(left[...], source[p % HALF], preferred_element_type=jnp.float32)
                + jnp.dot(left_early[...], from_core[p], preferred_element_type=jnp.float32)
            )
            copies.append(pltpu.make_async_copy(stage.at[p], out.at[:, columns], sems.at[p]))
            copies[-1].start()
        for copy in copies:
            copy.wait()


def finish(tail, left, left_early, from_x, from_z, from_core, held):
    rows = tail.shape[0]
    width, minutes = left.shape
    vmem, hbm = pl.BlockSpec(memory_space=pltpu.VMEM), pl.BlockSpec(memory_space=pltpu.HBM)
    return pl.pallas_call(
        finish_kernel,
        out_shape=jax.ShapeDtypeStruct(held.shape, held.dtype),
        in_specs=[vmem] * 6 + [hbm],
        out_specs=hbm,
        scratch_shapes=[
            pltpu.VMEM((PIECES, rows, width // PIECES), jnp.float32),
            pltpu.SemaphoreType.DMA((PIECES,)),
        ],
        input_output_aliases={6: 0},
        compiler_params=pltpu.CompilerParams(vmem_limit_bytes=10 * 1024 * 1024),
        cost_estimate=pl.CostEstimate(
            flops=2 * rows * width * minutes, bytes_accessed=4 * rows * width, transcendentals=0
        ),
    )(tail, left, left_early, from_x, from_z, from_core, held)


def local_planned(returns, prior):
    minutes, width = returns.shape
    rows, assets = prior.shape
    part = width // PIECES
    count = assets // width * PIECES
    hbm, vmem = pl.BlockSpec(memory_space=pltpu.HBM), pl.BlockSpec(memory_space=pltpu.VMEM)
    semaphores = [PIECES, 2, 4, 3 * PIECES + HALF, 3 * PIECES + HALF, 2 * PIECES, count]
    total, tail, left, left_early, hand, rest = pl.pallas_call(
        kernel,
        out_shape=(
            pltpu.VMEM((assets // width - 1, rows, width), jnp.float32),
            pltpu.VMEM((rows, width), jnp.float32),
            pltpu.VMEM((width, minutes), jnp.bfloat16),
            pltpu.VMEM((width, minutes), jnp.bfloat16),
            pltpu.HBM((HALF, minutes, part), jnp.bfloat16),
            pltpu.HBM((PIECES, minutes, part), jnp.bfloat16),
        ),
        in_specs=[hbm, hbm],
        out_specs=(vmem, vmem, vmem, vmem, hbm, hbm),
        scratch_shapes=[
            pltpu.VMEM((count, minutes, part), jnp.bfloat16),
            pltpu.VMEM((count, minutes, part), jnp.bfloat16),
            *[pltpu.SemaphoreType.DMA((n,)) for n in semaphores],
        ],
        compiler_params=pltpu.CompilerParams(
            collective_id=0, has_side_effects=True, vmem_limit_bytes=28 * 1024 * 1024
        ),
    )(pltpu.with_memory_space_constraint(returns, pltpu.HBM), prior)
    at = lambda row, column, core: (row * 2 + column) * 2 + core
    pairs_x = [(at(r, c, 1), at(r, 1 - c, 1)) for r in (0, 3) for c in (0, 1)]
    pairs_z = [(at(n, c, 1), at(r, c, 1)) for r, n in ((0, 1), (3, 2)) for c in (0, 1)]
    pairs_core = [(at(r, c, 0), at(r, c, 1)) for r in (0, 3) for c in (0, 1)]
    from_x = lax.ppermute(hand, ("assets", "tm"), pairs_x)
    from_z = lax.ppermute(hand, ("assets", "tm"), pairs_z)
    from_core = lax.ppermute(rest, ("assets", "tm"), pairs_core)
    return finish(tail, left, left_early, from_x, from_z, from_core, write_most(total))[None]


def solution(mesh):
    placed = (P("tm", ("groups", "assets")), P(("groups", "assets"), None))
    planned = mesh.shape["tm"] == 2 and mesh.shape["assets"] == 8

    def local(returns, prior):
        if planned and returns.shape[1] % (128 * PIECES) == 0 and returns.shape[0] % 128 == 0:
            return local_planned(returns, prior)
        return local_general(returns, prior)

    return jax.shard_map(
        local,
        mesh=mesh,
        in_specs=placed,
        out_specs=P("tm", ("groups", "assets"), None),
        check_vma=False,
    )
```

```python
import functools
import math

import jax
import jax.numpy as jnp
import numpy as np
from jax import lax
from jax.experimental import pallas as pl
from jax.experimental.pallas import tpu as pltpu
from jax.sharding import PartitionSpec as P

MESH = pl.DeviceIdType.MESH
PIECES = 4
HALF = PIECES // 2


def powers_of(minutes):
    lam = jnp.float32(0.9995)
    position = jnp.arange(minutes, dtype=jnp.float32)
    square = (jnp.float32(1.0) - lam) * jnp.power(lam, jnp.float32(minutes - 1) - position)
    return square, jnp.power(lam, jnp.float32(minutes))


def local_general(returns, prior):
    minutes, _ = returns.shape
    square, factor = powers_of(minutes)
    scaled = (returns.astype(jnp.float32) * jnp.sqrt(square)[:, None]).astype(jnp.bfloat16)
    tile = lax.dot_general(
        scaled,
        lax.all_gather(scaled, "assets", axis=1, tiled=True),
        (((0,), (0,)), ((), ())),
        preferred_element_type=jnp.float32,
    )
    mine = lax.axis_index("tm")
    everything = lax.all_gather(tile.astype(jnp.bfloat16), "tm")

    def turn(k, before):
        new = factor * before + everything[k].astype(jnp.float32)
        return jnp.where(k < mine, new, before)

    before = lax.fori_loop(0, lax.axis_size("tm"), turn, prior)
    return (factor * before + tile)[None]


def kernel(
    returns, prior, total, tail, left, left_early, hand, rest, mine, early,
    load_sem, prior_sem, send_sem, x_recv, z_recv, c_recv, f_recv
):
    minutes, width = returns.shape
    part = width // PIECES
    me, core = lax.axis_index("assets"), lax.axis_index("tm")
    row, column = me // 2, me % 2
    other = 1 - column
    upper = row // 2
    outer = jnp.logical_or(row == 0, row == 3)
    inner = jnp.logical_not(outer)
    first, second = core == 0, core == 1
    lam = float(np.float32(0.9995))
    factor = lam**minutes
    age = (minutes - 1) - lax.broadcasted_iota(jnp.int32, (1, minutes), 1)
    square = (1.0 - lam) * jnp.exp(age.astype(jnp.float32) * math.log(lam))
    line_row = lambda q: q + upper * (3 - 2 * q)
    block = lambda q, c: line_row(q) * 2 + c
    depth = (1 - upper) * row + upper * (3 - row)
    across = row * 2 + other
    beside = block(1 - depth, column)
    centre = (3 - row) * 2 + column

    barrier = pltpu.get_barrier_semaphore()
    for there in (across, beside):
        pl.semaphore_signal(barrier, 1, device_id={"assets": there}, device_id_type=MESH)
    pl.semaphore_signal(barrier, 1, device_id={"tm": 1 - core}, device_id_type=MESH)

    @pl.when(inner)
    def _():
        pl.semaphore_signal(barrier, 1, device_id={"assets": centre}, device_id_type=MESH)
        pl.semaphore_wait(barrier, 4)

    @pl.when(outer)
    def _():
        pl.semaphore_wait(barrier, 3)

    def remote(source, target, send, recv, where):
        return pltpu.make_async_remote_copy(
            src_ref=source, dst_ref=target, send_sem=send, recv_sem=recv,
            device_id=where, device_id_type=MESH,
        )

    def slot(j, p):
        return mine.at[j * PIECES + p]

    def send_x(source, j, p, k):
        remote(source, slot(j, p), send_sem.at[0], x_recv.at[k], {"assets": across}).start()

    def send_z(source, j, p, k):
        remote(source, slot(j, p), send_sem.at[1], z_recv.at[k], {"assets": beside}).start()

    def send_c(source, j, p, k):
        remote(source, slot(j, p), send_sem.at[2], c_recv.at[k], {"assets": centre}).start()

    def hand_on(source, j, p):
        k = j * PIECES + p

        @pl.when(first)
        def _():
            remote(source, early.at[k], send_sem.at[3], f_recv.at[k], {"tm": 1 - core}).start()

    def wait_recv(sem):
        pltpu.make_async_copy(mine.at[0], mine.at[0], sem).wait()

    def wait_all(sem, count):
        pieces = mine.at[pl.ds(0, count)]
        pltpu.make_async_copy(pieces, pieces, sem).wait()

    def got(sem, j, p):
        wait_recv(sem)
        hand_on(slot(j, p), j, p)

    own = lambda p: returns.at[:, pl.ds(p * part, part)]

    for p in range(PIECES):
        send_x(own(p), me, p, p)
        send_z(own(p), me, p, p)

        @pl.when(inner)
        def _():
            send_c(own(p), me, p, p)

        hand_on(own(p), me, p)
        pltpu.make_async_copy(own(p), slot(me, p), load_sem.at[0]).start()

    blocks = prior.shape[1] // width
    last = block(3, other)
    place_of = lambda j: (j + blocks - 1 - last) % blocks

    def prior_copy(k):
        j = (last + 1 + k) % blocks
        columns = pl.ds(pl.multiple_of(j * width, width), width)
        return pltpu.make_async_copy(prior.at[:, columns], total.at[k], prior_sem.at[0])

    tail_copy = pltpu.make_async_copy(
        prior.at[:, pl.ds(pl.multiple_of(last * width, width), width)], tail, prior_sem.at[1]
    )

    def start_prior(k, carry):
        prior_copy(k).start()
        return carry


    def prepare(p, carry):
        rows = pl.ds(pl.multiple_of(p * part, part), part)
        turned = mine[me * PIECES + p].astype(jnp.float32).T
        left[rows, :] = (turned * square).astype(jnp.bfloat16)

        @pl.when(second)
        def _():
            k = me * PIECES + p
            wait_recv(f_recv.at[k])
            turned = early[k].astype(jnp.float32).T
            left_early[rows, :] = (turned * (factor * square)).astype(jnp.bfloat16)

        return carry

    wait_all(load_sem.at[0], PIECES)
    lax.fori_loop(0, blocks - 1, start_prior, 0)
    tail_copy.start()
    lax.fori_loop(0, PIECES, prepare, 0)

    pltpu.make_async_copy(total, total, prior_sem.at[0]).wait()
    tail_copy.wait()

    def keep(j, p, k):
        return pltpu.make_async_copy(slot(j, p), hand.at[k], load_sem.at[0])

    def product(target, j, p, arrived=True):
        k = j * PIECES + p
        columns = pl.ds(pl.multiple_of(p * part, part), part)

        @pl.when(first)
        def _():
            target[:, columns] = factor * target[:, columns] + jnp.dot(
                left[...], mine[k], preferred_element_type=jnp.float32
            )

        @pl.when(second)
        def _():
            if arrived:
                wait_recv(f_recv.at[k])
            now = factor * factor * target[:, columns] + jnp.dot(
                left_early[...], early[k], preferred_element_type=jnp.float32
            )
            now += jnp.dot(left[...], mine[k], preferred_element_type=jnp.float32)
            target[:, columns] = now

    def own_product(p, carry):
        product(total.at[place_of(me)], me, p, arrived=False)
        return carry

    lax.fori_loop(0, PIECES, own_product, 0)

    @pl.when(outer)
    def _():
        def turn(k, carry):
            q, p = k // PIECES, k % PIECES
            jx, jz = block(q, other), block(1 + q, column)
            got(x_recv.at[k], jx, p)

            @pl.when(q == 0)
            def _():
                send_z(slot(jx, p), jx, p, PIECES + k)

            got(z_recv.at[k], jz, p)
            late = jnp.logical_and(k >= 2 * PIECES, k < 2 * PIECES + HALF)

            @pl.when(jnp.logical_or(k < 2 * PIECES, jnp.logical_and(late, first)))
            def _():
                send_x(slot(jz, p), jz, p, PIECES + k)

            @pl.when(jnp.logical_and(late, second))
            def _():
                keep(jz, p, p).start()

            product(total.at[place_of(jx)], jx, p)
            product(total.at[place_of(jz)], jz, p)
            return carry

        lax.fori_loop(0, 3 * PIECES, turn, 0)

        @pl.when(first)
        def _():
            j = block(3, other)

            for i in range(HALF):
                for sem, p in ((x_recv, i), (z_recv, HALF + i)):
                    wait_recv(sem.at[3 * PIECES + i])
                    pltpu.make_async_copy(slot(j, p), rest.at[p], load_sem.at[p]).start()
                for p in (i, HALF + i):
                    columns = pl.ds(p * part, part)
                    tail[:, columns] = factor * tail[:, columns] + jnp.dot(
                        left[...], mine[j * PIECES + p], preferred_element_type=jnp.float32
                    )
            for p in range(PIECES):
                wait_recv(load_sem.at[p])

        @pl.when(second)
        def _():
            def fade(p, carry):
                columns = pl.ds(pl.multiple_of(p * part, part), part)
                tail[:, columns] = factor * factor * tail[:, columns]
                return carry

            lax.fori_loop(0, PIECES, fade, 0)

    @pl.when(inner)
    def _():
        def turn(k, carry):
            q, p = k // PIECES, k % PIECES
            jx, jz, jc = block(1 + q, other), block(0, (column + q) % 2), block(2 + q, column)
            got(c_recv.at[k], jc, p)
            send_z(slot(jc, p), jc, p, PIECES + k)
            send_x(slot(jc, p), jc, p, PIECES + k + q * HALF * (1 - 2 * (p // HALF)))
            got(z_recv.at[k], jz, p)

            @pl.when(q == 0)
            def _():
                send_c(slot(jz, p), jz, p, PIECES + k)

            got(x_recv.at[k], jx, p)
            product(total.at[place_of(jc)], jc, p)
            product(total.at[place_of(jz)], jz, p)
            product(total.at[place_of(jx)], jx, p)
            return carry

        lax.fori_loop(0, 2 * PIECES, turn, 0)

        def end(k, carry):
            j, p = block(3, other), (k + HALF) % PIECES
            got(x_recv.at[2 * PIECES + k], j, p)

            @pl.when(jnp.logical_and(k < HALF, first))
            def _():
                send_z(slot(j, p), j, p, 3 * PIECES + k)

            @pl.when(jnp.logical_and(k < HALF, second))
            def _():
                keep(j, p, k).start()

            product(tail, j, p)
            return carry

        lax.fori_loop(0, PIECES, end, 0)

    @pl.when(outer)
    def _():
        wait_all(send_sem.at[1], 2 * PIECES)
        pl.when(first)(lambda: wait_all(send_sem.at[0], 3 * PIECES + HALF))
        pl.when(second)(lambda: wait_all(send_sem.at[0], 3 * PIECES))

    @pl.when(inner)
    def _():
        wait_all(send_sem.at[0], 3 * PIECES)
        wait_all(send_sem.at[2], 2 * PIECES)
        pl.when(first)(lambda: wait_all(send_sem.at[1], 3 * PIECES + HALF))
        pl.when(second)(lambda: wait_all(send_sem.at[1], 3 * PIECES))

    pl.when(jnp.logical_and(first, outer))(lambda: wait_all(send_sem.at[3], (blocks - 1) * PIECES))
    pl.when(jnp.logical_and(first, inner))(lambda: wait_all(send_sem.at[3], blocks * PIECES))
    pl.when(second)(lambda: wait_all(load_sem.at[0], HALF))


def place():
    me = lax.axis_index("assets")
    row, column = me // 2, me % 2
    upper = row // 2
    outer = jnp.logical_or(row == 0, row == 3)
    last = 3 * (1 - upper) * 2 + 1 - column
    return outer, last


def write_kernel(total, out, sems):
    width = total.shape[2]
    blocks = out.shape[1] // width
    _, last = place()

    def piece(k):
        columns = pl.ds(pl.multiple_of((last + 1 + k) % blocks * width, width), width)
        return pltpu.make_async_copy(total.at[k], out.at[:, columns], sems.at[k])

    for k in range(blocks - 1):
        piece(k).start()
    for k in range(blocks - 1):
        piece(k).wait()


def write_most(total):
    blocks, rows, width = total.shape
    assets = (blocks + 1) * width
    return pl.pallas_call(
        write_kernel,
        out_shape=jax.ShapeDtypeStruct((rows, assets), total.dtype),
        in_specs=[pl.BlockSpec(memory_space=pltpu.VMEM)],
        out_specs=pl.BlockSpec(memory_space=pltpu.HBM),
        scratch_shapes=[pltpu.SemaphoreType.DMA((blocks,))],
        compiler_params=pltpu.CompilerParams(vmem_limit_bytes=1024 * 1024),
        cost_estimate=pl.CostEstimate(
            flops=0, bytes_accessed=8 * rows * assets, transcendentals=0
        ),
    )(total)


def finish_kernel(tail, left, left_early, from_x, from_z, from_core, held, out, stage, sems):
    width, part = left.shape[0], from_x.shape[2]
    outer, last = place()
    late = jnp.logical_and(outer, lax.axis_index("tm") == 1)
    start = pl.multiple_of(last * width, width)

    @pl.when(jnp.logical_not(late))
    def _():
        columns = pl.ds(start, width)
        copy = pltpu.make_async_copy(tail, out.at[:, columns], sems.at[0])
        copy.start()
        copy.wait()

    @pl.when(late)
    def _():
        copies = []
        for p in range(PIECES):
            source = from_x if p < HALF else from_z
            columns = pl.ds(pl.multiple_of(start + p * part, part), part)
            stage[p] = (
                tail[:, pl.ds(p * part, part)]
                + jnp.dot(left[...], source[p % HALF], preferred_element_type=jnp.float32)
                + jnp.dot(left_early[...], from_core[p], preferred_element_type=jnp.float32)
            )
            copies.append(pltpu.make_async_copy(stage.at[p], out.at[:, columns], sems.at[p]))
            copies[-1].start()
        for copy in copies:
            copy.wait()


def finish(tail, left, left_early, from_x, from_z, from_core, held):
    rows = tail.shape[0]
    width, minutes = left.shape
    vmem, hbm = pl.BlockSpec(memory_space=pltpu.VMEM), pl.BlockSpec(memory_space=pltpu.HBM)
    return pl.pallas_call(
        finish_kernel,
        out_shape=jax.ShapeDtypeStruct(held.shape, held.dtype),
        in_specs=[vmem] * 6 + [hbm],
        out_specs=hbm,
        scratch_shapes=[
            pltpu.VMEM((PIECES, rows, width // PIECES), jnp.float32),
            pltpu.SemaphoreType.DMA((PIECES,)),
        ],
        input_output_aliases={6: 0},
        compiler_params=pltpu.CompilerParams(vmem_limit_bytes=10 * 1024 * 1024),
        cost_estimate=pl.CostEstimate(
            flops=2 * rows * width * minutes, bytes_accessed=4 * rows * width, transcendentals=0
        ),
    )(tail, left, left_early, from_x, from_z, from_core, held)


def local_planned(returns, prior):
    minutes, width = returns.shape
    rows, assets = prior.shape
    part = width // PIECES
    count = assets // width * PIECES
    hbm, vmem = pl.BlockSpec(memory_space=pltpu.HBM), pl.BlockSpec(memory_space=pltpu.VMEM)
    semaphores = [PIECES, 2, 4, 3 * PIECES + HALF, 3 * PIECES + HALF, 2 * PIECES, count]
    total, tail, left, left_early, hand, rest = pl.pallas_call(
        kernel,
        out_shape=(
            pltpu.VMEM((assets // width - 1, rows, width), jnp.float32),
            pltpu.VMEM((rows, width), jnp.float32),
            pltpu.VMEM((width, minutes), jnp.bfloat16),
            pltpu.VMEM((width, minutes), jnp.bfloat16),
            pltpu.HBM((HALF, minutes, part), jnp.bfloat16),
            pltpu.HBM((PIECES, minutes, part), jnp.bfloat16),
        ),
        in_specs=[hbm, hbm],
        out_specs=(vmem, vmem, vmem, vmem, hbm, hbm),
        scratch_shapes=[
            pltpu.VMEM((count, minutes, part), jnp.bfloat16),
            pltpu.VMEM((count, minutes, part), jnp.bfloat16),
            *[pltpu.SemaphoreType.DMA((n,)) for n in semaphores],
        ],
        compiler_params=pltpu.CompilerParams(
            collective_id=0, has_side_effects=True, vmem_limit_bytes=28 * 1024 * 1024
        ),
    )(pltpu.with_memory_space_constraint(returns, pltpu.HBM), prior)
    at = lambda row, column, core: (row * 2 + column) * 2 + core
    pairs_x = [(at(r, c, 1), at(r, 1 - c, 1)) for r in (0, 3) for c in (0, 1)]
    pairs_z = [(at(n, c, 1), at(r, c, 1)) for r, n in ((0, 1), (3, 2)) for c in (0, 1)]
    pairs_core = [(at(r, c, 0), at(r, c, 1)) for r in (0, 3) for c in (0, 1)]
    from_x = lax.ppermute(hand, ("assets", "tm"), pairs_x)
    from_z = lax.ppermute(hand, ("assets", "tm"), pairs_z)
    from_core = lax.ppermute(rest, ("assets", "tm"), pairs_core)
    return finish(tail, left, left_early, from_x, from_z, from_core, write_most(total))[None]


def solution(mesh):
    placed = (P("tm", ("groups", "assets")), P(("groups", "assets"), None))
    planned = mesh.shape["tm"] == 2 and mesh.shape["assets"] == 8

    def local(returns, prior):
        if planned and returns.shape[1] % (128 * PIECES) == 0 and returns.shape[0] % 128 == 0:
            return local_planned(returns, prior)
        return local_general(returns, prior)

    return jax.shard_map(
        local,
        mesh=mesh,
        in_specs=placed,
        out_specs=P("tm", ("groups", "assets"), None),
        check_vma=False,
    )
```

```python
import functools
import math

import jax
import jax.numpy as jnp
import numpy as np
from jax import lax
from jax.experimental import pallas as pl
from jax.experimental.pallas import tpu as pltpu
from jax.sharding import PartitionSpec as P

MESH = pl.DeviceIdType.MESH
PIECES = 4
HALF = PIECES // 2


def powers_of(minutes):
    lam = jnp.float32(0.9995)
    position = jnp.arange(minutes, dtype=jnp.float32)
    square = (jnp.float32(1.0) - lam) * jnp.power(lam, jnp.float32(minutes - 1) - position)
    return square, jnp.power(lam, jnp.float32(minutes))


def local_general(returns, prior):
    minutes, _ = returns.shape
    square, factor = powers_of(minutes)
    scaled = (returns.astype(jnp.float32) * jnp.sqrt(square)[:, None]).astype(jnp.bfloat16)
    tile = lax.dot_general(
        scaled,
        lax.all_gather(scaled, "assets", axis=1, tiled=True),
        (((0,), (0,)), ((), ())),
        preferred_element_type=jnp.float32,
    )
    mine = lax.axis_index("tm")
    everything = lax.all_gather(tile.astype(jnp.bfloat16), "tm")

    def turn(k, before):
        new = factor * before + everything[k].astype(jnp.float32)
        return jnp.where(k < mine, new, before)

    before = lax.fori_loop(0, lax.axis_size("tm"), turn, prior)
    return (factor * before + tile)[None]


def kernel(
    returns, prior, total, tail, left, left_early, hand, rest, mine, early,
    load_sem, prior_sem, send_sem, x_recv, z_recv, c_recv, f_recv
):
    minutes, width = returns.shape
    part = width // PIECES
    me, core = lax.axis_index("assets"), lax.axis_index("tm")
    row, column = me // 2, me % 2
    other = 1 - column
    upper = row // 2
    outer = jnp.logical_or(row == 0, row == 3)
    inner = jnp.logical_not(outer)
    first, second = core == 0, core == 1
    lam = float(np.float32(0.9995))
    factor = lam**minutes
    age = (minutes - 1) - lax.broadcasted_iota(jnp.int32, (1, minutes), 1)
    square = (1.0 - lam) * jnp.exp(age.astype(jnp.float32) * math.log(lam))
    line_row = lambda q: q + upper * (3 - 2 * q)
    block = lambda q, c: line_row(q) * 2 + c
    depth = (1 - upper) * row + upper * (3 - row)
    across = row * 2 + other
    beside = block(1 - depth, column)
    centre = (3 - row) * 2 + column

    barrier = pltpu.get_barrier_semaphore()
    for there in (across, beside):
        pl.semaphore_signal(barrier, 1, device_id={"assets": there}, device_id_type=MESH)
    pl.semaphore_signal(barrier, 1, device_id={"tm": 1 - core}, device_id_type=MESH)

    @pl.when(inner)
    def _():
        pl.semaphore_signal(barrier, 1, device_id={"assets": centre}, device_id_type=MESH)
        pl.semaphore_wait(barrier, 4)

    @pl.when(outer)
    def _():
        pl.semaphore_wait(barrier, 3)

    def remote(source, target, send, recv, where):
        return pltpu.make_async_remote_copy(
            src_ref=source, dst_ref=target, send_sem=send, recv_sem=recv,
            device_id=where, device_id_type=MESH,
        )

    def slot(j, p):
        return mine.at[j * PIECES + p]

    def send_x(source, j, p, k):
        remote(source, slot(j, p), send_sem.at[0], x_recv.at[k], {"assets": across}).start()

    def send_z(source, j, p, k):
        remote(source, slot(j, p), send_sem.at[1], z_recv.at[k], {"assets": beside}).start()

    def send_c(source, j, p, k):
        remote(source, slot(j, p), send_sem.at[2], c_recv.at[k], {"assets": centre}).start()

    def hand_on(source, j, p):
        k = j * PIECES + p

        @pl.when(first)
        def _():
            remote(source, early.at[k], send_sem.at[3], f_recv.at[k], {"tm": 1 - core}).start()

    def wait_recv(sem):
        pltpu.make_async_copy(mine.at[0], mine.at[0], sem).wait()

    def wait_all(sem, count):
        pieces = mine.at[pl.ds(0, count)]
        pltpu.make_async_copy(pieces, pieces, sem).wait()

    def got(sem, j, p):
        wait_recv(sem)
        hand_on(slot(j, p), j, p)

    own = lambda p: returns.at[:, pl.ds(p * part, part)]

    for p in range(PIECES):
        send_x(own(p), me, p, p)
        send_z(own(p), me, p, p)

        @pl.when(inner)
        def _():
            send_c(own(p), me, p, p)

        hand_on(own(p), me, p)
        pltpu.make_async_copy(own(p), slot(me, p), load_sem.at[0]).start()

    blocks = prior.shape[1] // width
    last = block(3, other)
    place_of = lambda j: (j + blocks - 1 - last) % blocks

    def prior_copy(k):
        j = (last + 1 + k) % blocks
        columns = pl.ds(pl.multiple_of(j * width, width), width)
        return pltpu.make_async_copy(prior.at[:, columns], total.at[k], prior_sem.at[0])

    tail_copy = pltpu.make_async_copy(
        prior.at[:, pl.ds(pl.multiple_of(last * width, width), width)], tail, prior_sem.at[1]
    )

    def start_prior(k, carry):
        prior_copy(k).start()
        return carry


    def prepare(p, carry):
        rows = pl.ds(pl.multiple_of(p * part, part), part)
        turned = mine[me * PIECES + p].astype(jnp.float32).T
        left[rows, :] = (turned * square).astype(jnp.bfloat16)

        @pl.when(second)
        def _():
            k = me * PIECES + p
            wait_recv(f_recv.at[k])
            turned = early[k].astype(jnp.float32).T
            left_early[rows, :] = (turned * (factor * square)).astype(jnp.bfloat16)

        return carry

    wait_all(load_sem.at[0], PIECES)
    lax.fori_loop(0, blocks - 1, start_prior, 0)
    tail_copy.start()
    lax.fori_loop(0, PIECES, prepare, 0)

    pltpu.make_async_copy(total, total, prior_sem.at[0]).wait()
    tail_copy.wait()

    def keep(j, p, k):
        return pltpu.make_async_copy(slot(j, p), hand.at[k], load_sem.at[0])

    def product(target, j, p, arrived=True):
        k = j * PIECES + p
        columns = pl.ds(pl.multiple_of(p * part, part), part)

        @pl.when(first)
        def _():
            target[:, columns] = factor * target[:, columns] + jnp.dot(
                left[...], mine[k], preferred_element_type=jnp.float32
            )

        @pl.when(second)
        def _():
            if arrived:
                wait_recv(f_recv.at[k])
            now = factor * factor * target[:, columns] + jnp.dot(
                left_early[...], early[k], preferred_element_type=jnp.float32
            )
            now += jnp.dot(left[...], mine[k], preferred_element_type=jnp.float32)
            target[:, columns] = now

    def own_product(p, carry):
        product(total.at[place_of(me)], me, p, arrived=False)
        return carry

    lax.fori_loop(0, PIECES, own_product, 0)

    @pl.when(outer)
    def _():
        def turn(k, carry):
            q, p = k // PIECES, k % PIECES
            jx, jz = block(q, other), block(1 + q, column)
            got(x_recv.at[k], jx, p)

            @pl.when(q == 0)
            def _():
                send_z(slot(jx, p), jx, p, PIECES + k)

            got(z_recv.at[k], jz, p)
            late = jnp.logical_and(k >= 2 * PIECES, k < 2 * PIECES + HALF)

            @pl.when(jnp.logical_or(k < 2 * PIECES, jnp.logical_and(late, first)))
            def _():
                send_x(slot(jz, p), jz, p, PIECES + k)

            @pl.when(jnp.logical_and(late, second))
            def _():
                keep(jz, p, p).start()

            product(total.at[place_of(jx)], jx, p)
            product(total.at[place_of(jz)], jz, p)
            return carry

        lax.fori_loop(0, 3 * PIECES, turn, 0)

        @pl.when(first)
        def _():
            j = block(3, other)

            for i in range(HALF):
                for sem, p in ((x_recv, i), (z_recv, HALF + i)):
                    wait_recv(sem.at[3 * PIECES + i])
                    pltpu.make_async_copy(slot(j, p), rest.at[p], load_sem.at[0]).start()
                for p in (i, HALF + i):
                    columns = pl.ds(p * part, part)
                    tail[:, columns] = factor * tail[:, columns] + jnp.dot(
                        left[...], mine[j * PIECES + p], preferred_element_type=jnp.float32
                    )
            wait_all(load_sem.at[0], PIECES)

        @pl.when(second)
        def _():
            def fade(p, carry):
                columns = pl.ds(pl.multiple_of(p * part, part), part)
                tail[:, columns] = factor * factor * tail[:, columns]
                return carry

            lax.fori_loop(0, PIECES, fade, 0)

    @pl.when(inner)
    def _():
        def turn(k, carry):
            q, p = k // PIECES, k % PIECES
            jx, jz, jc = block(1 + q, other), block(0, (column + q) % 2), block(2 + q, column)
            got(c_recv.at[k], jc, p)
            send_z(slot(jc, p), jc, p, PIECES + k)
            send_x(slot(jc, p), jc, p, PIECES + k + q * HALF * (1 - 2 * (p // HALF)))
            got(z_recv.at[k], jz, p)

            @pl.when(q == 0)
            def _():
                send_c(slot(jz, p), jz, p, PIECES + k)

            got(x_recv.at[k], jx, p)
            product(total.at[place_of(jc)], jc, p)
            product(total.at[place_of(jz)], jz, p)
            product(total.at[place_of(jx)], jx, p)
            return carry

        lax.fori_loop(0, 2 * PIECES, turn, 0)

        def end(k, carry):
            j, p = block(3, other), (k + HALF) % PIECES
            got(x_recv.at[2 * PIECES + k], j, p)

            @pl.when(jnp.logical_and(k < HALF, first))
            def _():
                send_z(slot(j, p), j, p, 3 * PIECES + k)

            @pl.when(jnp.logical_and(k < HALF, second))
            def _():
                keep(j, p, k).start()

            product(tail, j, p)
            return carry

        lax.fori_loop(0, PIECES, end, 0)

    @pl.when(outer)
    def _():
        wait_all(send_sem.at[1], 2 * PIECES)
        pl.when(first)(lambda: wait_all(send_sem.at[0], 3 * PIECES + HALF))
        pl.when(second)(lambda: wait_all(send_sem.at[0], 3 * PIECES))

    @pl.when(inner)
    def _():
        wait_all(send_sem.at[0], 3 * PIECES)
        wait_all(send_sem.at[2], 2 * PIECES)
        pl.when(first)(lambda: wait_all(send_sem.at[1], 3 * PIECES + HALF))
        pl.when(second)(lambda: wait_all(send_sem.at[1], 3 * PIECES))

    pl.when(jnp.logical_and(first, outer))(lambda: wait_all(send_sem.at[3], (blocks - 1) * PIECES))
    pl.when(jnp.logical_and(first, inner))(lambda: wait_all(send_sem.at[3], blocks * PIECES))
    pl.when(second)(lambda: wait_all(load_sem.at[0], HALF))


def place():
    me = lax.axis_index("assets")
    row, column = me // 2, me % 2
    upper = row // 2
    outer = jnp.logical_or(row == 0, row == 3)
    last = 3 * (1 - upper) * 2 + 1 - column
    return outer, last


def write_kernel(total, out, sems):
    width = total.shape[2]
    blocks = out.shape[1] // width
    _, last = place()

    def piece(k):
        columns = pl.ds(pl.multiple_of((last + 1 + k) % blocks * width, width), width)
        return pltpu.make_async_copy(total.at[k], out.at[:, columns], sems.at[k])

    for k in range(blocks - 1):
        piece(k).start()
    for k in range(blocks - 1):
        piece(k).wait()


def write_most(total):
    blocks, rows, width = total.shape
    assets = (blocks + 1) * width
    return pl.pallas_call(
        write_kernel,
        out_shape=jax.ShapeDtypeStruct((rows, assets), total.dtype),
        in_specs=[pl.BlockSpec(memory_space=pltpu.VMEM)],
        out_specs=pl.BlockSpec(memory_space=pltpu.HBM),
        scratch_shapes=[pltpu.SemaphoreType.DMA((blocks,))],
        compiler_params=pltpu.CompilerParams(vmem_limit_bytes=1024 * 1024),
        cost_estimate=pl.CostEstimate(
            flops=0, bytes_accessed=8 * rows * assets, transcendentals=0
        ),
    )(total)


def finish_kernel(tail, left, left_early, from_x, from_z, from_core, held, out, stage, sems):
    width, part = left.shape[0], from_x.shape[2]
    outer, last = place()
    late = jnp.logical_and(outer, lax.axis_index("tm") == 1)
    start = pl.multiple_of(last * width, width)

    @pl.when(jnp.logical_not(late))
    def _():
        columns = pl.ds(start, width)
        copy = pltpu.make_async_copy(tail, out.at[:, columns], sems.at[0])
        copy.start()
        copy.wait()

    @pl.when(late)
    def _():
        copies = []
        for p in range(PIECES):
            source = from_x if p < HALF else from_z
            columns = pl.ds(pl.multiple_of(start + p * part, part), part)
            stage[p] = (
                tail[:, pl.ds(p * part, part)]
                + jnp.dot(left[...], source[p % HALF], preferred_element_type=jnp.float32)
                + jnp.dot(left_early[...], from_core[p], preferred_element_type=jnp.float32)
            )
            copies.append(pltpu.make_async_copy(stage.at[p], out.at[:, columns], sems.at[p]))
            copies[-1].start()
        for copy in copies:
            copy.wait()


def finish(tail, left, left_early, from_x, from_z, from_core, held):
    rows = tail.shape[0]
    width, minutes = left.shape
    vmem, hbm = pl.BlockSpec(memory_space=pltpu.VMEM), pl.BlockSpec(memory_space=pltpu.HBM)
    return pl.pallas_call(
        finish_kernel,
        out_shape=jax.ShapeDtypeStruct(held.shape, held.dtype),
        in_specs=[vmem] * 6 + [hbm],
        out_specs=hbm,
        scratch_shapes=[
            pltpu.VMEM((PIECES, rows, width // PIECES), jnp.float32),
            pltpu.SemaphoreType.DMA((PIECES,)),
        ],
        input_output_aliases={6: 0},
        compiler_params=pltpu.CompilerParams(vmem_limit_bytes=10 * 1024 * 1024),
        cost_estimate=pl.CostEstimate(
            flops=2 * rows * width * minutes, bytes_accessed=4 * rows * width, transcendentals=0
        ),
    )(tail, left, left_early, from_x, from_z, from_core, held)


def local_planned(returns, prior):
    minutes, width = returns.shape
    rows, assets = prior.shape
    part = width // PIECES
    count = assets // width * PIECES
    hbm, vmem = pl.BlockSpec(memory_space=pltpu.HBM), pl.BlockSpec(memory_space=pltpu.VMEM)
    semaphores = [1, 2, 4, 3 * PIECES + HALF, 3 * PIECES + HALF, 2 * PIECES, count]
    total, tail, left, left_early, hand, rest = pl.pallas_call(
        kernel,
        out_shape=(
            pltpu.VMEM((assets // width - 1, rows, width), jnp.float32),
            pltpu.VMEM((rows, width), jnp.float32),
            pltpu.VMEM((width, minutes), jnp.bfloat16),
            pltpu.VMEM((width, minutes), jnp.bfloat16),
            pltpu.HBM((HALF, minutes, part), jnp.bfloat16),
            pltpu.HBM((PIECES, minutes, part), jnp.bfloat16),
        ),
        in_specs=[hbm, hbm],
        out_specs=(vmem, vmem, vmem, vmem, hbm, hbm),
        scratch_shapes=[
            pltpu.VMEM((count, minutes, part), jnp.bfloat16),
            pltpu.VMEM((count, minutes, part), jnp.bfloat16),
            *[pltpu.SemaphoreType.DMA((n,)) for n in semaphores],
        ],
        compiler_params=pltpu.CompilerParams(
            collective_id=0, has_side_effects=True, vmem_limit_bytes=28 * 1024 * 1024
        ),
    )(pltpu.with_memory_space_constraint(returns, pltpu.HBM), prior)
    at = lambda row, column, core: (row * 2 + column) * 2 + core
    pairs_x = [(at(r, c, 1), at(r, 1 - c, 1)) for r in (0, 3) for c in (0, 1)]
    pairs_z = [(at(n, c, 1), at(r, c, 1)) for r, n in ((0, 1), (3, 2)) for c in (0, 1)]
    pairs_core = [(at(r, c, 0), at(r, c, 1)) for r in (0, 3) for c in (0, 1)]
    from_x = lax.ppermute(hand, ("assets", "tm"), pairs_x)
    from_z = lax.ppermute(hand, ("assets", "tm"), pairs_z)
    from_core = lax.ppermute(rest, ("assets", "tm"), pairs_core)
    return finish(tail, left, left_early, from_x, from_z, from_core, write_most(total))[None]


def solution(mesh):
    placed = (P("tm", ("groups", "assets")), P(("groups", "assets"), None))
    planned = mesh.shape["tm"] == 2 and mesh.shape["assets"] == 8

    def local(returns, prior):
        if planned and returns.shape[1] % (128 * PIECES) == 0 and returns.shape[0] % 128 == 0:
            return local_planned(returns, prior)
        return local_general(returns, prior)

    return jax.shard_map(
        local,
        mesh=mesh,
        in_specs=placed,
        out_specs=P("tm", ("groups", "assets"), None),
        check_vma=False,
    )
```
